32 devices in a mesh: region: 2 (over x), blk: 16 (over z, y, core).
Axes of the slice: x: 2, y: 2, z: 4, core: 2. Of those that a mesh axis runs over, the one named last changes fastest.
Arguments:
- ensemble: float32 [64, 256, 128], P(('region', 'blk'))
- observed: float32 [64, 256, 128], P(('region', 'blk')), may hold values from -6 to 6
- obs_var: float32 [64, 256], P(('region', 'blk')), may hold values from 0.5 to 2
- ridge: float32 [64], P(('region', 'blk')), may hold values from 0.05 to 0.5
- pred_back: int32 [64, 12], P(('region', 'blk')), may hold values from 0 to 16, as said below
- bounds: float32 [2], replicated, may hold values from 0.2 to 6, as said below
Outputs:
- analysis: float32 [64, 256, 128], P(('region', 'blk'))
The draws below stay inside these ranges and needn't reach their ends.
Inputs may be any that keep to these rules, and one draw needn't show every extreme that they name: `pred_back`: each row holds distinct distances among 1 to 16, never more than the block's own index, with 0 for an empty slot; the last block fills all 12 slots. bounds[0] < bounds[1].
All inputs are finite; a program needn't handle non-finite values.
Results may differ from the reference program's by a relative error of at most 0.0003.
Values sent between devices are 32-bit elements; how exact they have to be, the bound alone decides.
A program may use at most 192 MiB of HBM per device.

```python
import math
import jax
import jax.numpy as jnp
from jax import lax

M = 128
ROWS = 256
SLOTS = 12
REACH = 16
ITERS = 3
NBLK = 64


def draw_ensemble(key, part):
    first = jax.random.fold_in(jax.random.fold_in(key, 11), 0)
    noise = jax.random.normal(first, (NBLK, ROWS, M), jnp.float32)

    def advance(carry, fresh):
        state = 0.8 * carry + 0.6 * fresh
        return (state, state)
    start = jnp.zeros((ROWS, M), jnp.float32)
    unused, analysis_output = lax.scan(advance, start, noise)
    return analysis_output


def draw_pred_back(key, part):
    first, second, third = jax.random.split(jax.random.fold_in(key, 23), 3)
    scores = jax.random.randint(first, (NBLK, REACH), 0, 1 << 20) * REACH + jnp.arange(REACH, dtype=jnp.int32)[None, :]
    order = jnp.argsort(scores, axis=1).astype(jnp.int32)
    distance = order[:, :SLOTS] + 1
    base = jax.random.randint(second, (NBLK,), 1, 8)
    many = jax.random.randint(third, (NBLK,), 0, 8) == 0
    blocks = jnp.arange(NBLK, dtype=jnp.int32)
    count = jnp.where(many | (blocks == NBLK - 1), SLOTS, base)
    slot_index = jnp.arange(SLOTS, dtype=jnp.int32)
    chosen = jnp.where(slot_index[None, :] < count[:, None], distance, 0)
    chosen = jnp.where(chosen <= blocks[:, None], chosen, 0)
    return chosen.astype(jnp.int32)


def draw_bounds(key, part):
    first, second = jax.random.split(jax.random.fold_in(key, 37))
    lower_bound = jax.random.uniform(first, (1,), jnp.float32, 0.2, 0.5)
    upper_bound = jax.random.uniform(second, (1,), jnp.float32, 3.0, 6.0)
    return jnp.concatenate([lower_bound, upper_bound])


def shard_levels(stream_key, dims, cuts, smallest, largest):
    gain = 1.0
    for axis_at, parts in cuts:
        heights = jax.random.uniform(jax.random.fold_in(jax.random.fold_in(stream_key, 6), axis_at), (parts,), jnp.float32, smallest / len(cuts), largest / len(cuts))
        gain = gain * jnp.repeat(jnp.exp(heights), dims[axis_at] // parts).reshape((-1,) + (1,) * (len(dims) - 1 - axis_at))
    return gain


def normal_values(rng, extent, spread, bound, cuts=(), held_as=jnp.bfloat16):
    result = spread * jax.random.normal(rng, extent, jnp.float32)
    if cuts:
        result = result * shard_levels(rng, extent, cuts, -0.22, 0.18)
    return jnp.clip(result, -bound, bound).astype(held_as)


def setup_inputs(seed: int = 0) -> dict:
    arg_keys = jax.random.split(jax.random.key(seed), 7)
    ensemble = draw_ensemble(jax.random.fold_in(arg_keys[6], 71), 0)
    observed = normal_values(arg_keys[1], (NBLK, ROWS, M), 1.0, 6.0, ((0, 32),), jnp.float32)
    obs_var = jnp.clip(jnp.exp(math.log(2.0) - 1.3862944 * jax.random.uniform(arg_keys[2], (NBLK, ROWS), jnp.float32) ** shard_levels(arg_keys[2], (NBLK, ROWS), ((0, 32),), -0.2, 0.2)), 0.5, 2.0)
    ridge = jnp.clip(jnp.exp(math.log(0.5) - 2.3025851 * jax.random.uniform(arg_keys[3], (NBLK,), jnp.float32) ** shard_levels(arg_keys[3], (NBLK,), ((0, 32),), -0.2, 0.2)), 0.05, 0.5)
    pred_back = draw_pred_back(jax.random.fold_in(arg_keys[6], 71), 0)
    bounds = draw_bounds(jax.random.fold_in(arg_keys[6], 71), 0)
    return {"ensemble": ensemble, "observed": observed, "obs_var": obs_var, "ridge": ridge, "pred_back": pred_back, "bounds": bounds}


def small_solve(gram, target):
    size = gram.shape[0]
    factor = {}
    for block_position in range(size):
        running = gram[block_position, block_position]
        for k in range(block_position):
            running = running - factor[block_position, k] * factor[block_position, k]
        factor[block_position, block_position] = jnp.sqrt(running)
        for i in range(block_position + 1, size):
            running = gram[i, block_position]
            for k in range(block_position):
                running = running - factor[i, k] * factor[block_position, k]
            factor[i, block_position] = running / factor[block_position, block_position]
    forward = []
    for i in range(size):
        running = target[i]
        for k in range(i):
            running = running - factor[i, k] * forward[k]
        forward.append(running / factor[i, i])
    analysis_output = [None] * size
    for i in reversed(range(size)):
        running = forward[i]
        for k in range(i + 1, size):
            running = running - factor[k, i] * analysis_output[k]
        analysis_output[i] = running / factor[i, i]
    return jnp.stack(analysis_output)

def reference(ensemble, observed, obs_var, ridge, pred_back, bounds):
    highest = lax.Precision.HIGHEST
    nblocks = ensemble.shape[0]
    members = ensemble.shape[2]
    slots = pred_back.shape[1]
    anomaly = (ensemble - lax.optimization_barrier(jnp.mean(ensemble, axis=2, keepdims=True))) / jnp.sqrt(jnp.float32(members - 1))
    empty_zero_matrix = jnp.zeros((1,) + ensemble.shape[1:], ensemble.dtype)
    padded = jnp.concatenate([anomaly, empty_zero_matrix], axis=0)
    block_index_list = jnp.arange(nblocks, dtype=jnp.int32)[:, None] - pred_back
    block_index_list = jnp.where(pred_back > 0, block_index_list, nblocks).astype(jnp.int32)
    identity = jnp.eye(slots, dtype=jnp.float32)

    def regress(inputs):
        own, picked, weight = inputs
        preds = padded[picked]
        gram = jnp.einsum('jrm,krm->jkr', preds, preds, precision=highest) + weight * identity[:, :, None]
        target = jnp.einsum('jrm,rm->jr', preds, own, precision=highest)
        regression_coefficients = small_solve(gram, target)
        resid = own - jnp.einsum('jr,jrm->rm', regression_coefficients, preds, precision=highest)
        return (regression_coefficients, lax.optimization_barrier(jnp.sum(resid * resid, axis=1)) + 1e-05)
    regression_coefficients, dvar = lax.map(regress, (anomaly, block_index_list, ridge))

    def lower(entry_values):
        padded_entry_values = jnp.concatenate([entry_values, empty_zero_matrix], axis=0)
        analysis_output = entry_values
        for block_position in range(slots):
            analysis_output = analysis_output - regression_coefficients[:, block_position, :, None] * padded_entry_values[block_index_list[:, block_position]]
        return analysis_output

    def upper(entry_values):
        analysis_output = jnp.concatenate([entry_values, empty_zero_matrix], axis=0)
        for block_position in range(slots):
            analysis_output = analysis_output.at[block_index_list[:, block_position]].add(-regression_coefficients[:, block_position, :, None] * entry_values)
        return analysis_output[:nblocks]
    inverse_obs = 1.0 / obs_var

    def operator(entry_values):
        return upper(lower(entry_values) / dvar[:, :, None]) + inverse_obs[:, :, None] * entry_values
    lower_bound = bounds[0]
    upper_bound = bounds[1]
    theta = (upper_bound + lower_bound) / 2
    delta = (upper_bound - lower_bound) / 2
    sigma = theta / delta
    rho_now = 1.0 / sigma
    residue = inverse_obs[:, :, None] * (observed - ensemble)
    increment = jnp.zeros_like(ensemble)
    direction = residue / theta
    for step in range(ITERS):
        increment = increment + direction
        residue = residue - operator(direction)
        rho_next = 1.0 / (2 * sigma - rho_now)
        direction = rho_next * rho_now * direction + 2 * rho_next / delta * residue
        rho_now = rho_next
    increment = increment + direction
    return ensemble + increment
```

```python
import functools
import math

import jax
import jax.numpy as jnp
from jax import lax
from jax.experimental import pallas as pl
from jax.experimental.pallas import tpu as pltpu
from jax.sharding import PartitionSpec as P

REACH = 16
ITERS = 3


def from_behind(value, axis, steps):
    count = lax.axis_size(axis)
    first, last = (max(0, -steps), min(count, count - steps))
    return lax.ppermute(value, axis, [(source, source + steps) for source in range(first, last)])


def small_solve(gram, target):
    size = gram.shape[0]
    factor = {}
    for block_position in range(size):
        running = gram[block_position, block_position]
        for k in range(block_position):
            running = running - factor[block_position, k] * factor[block_position, k]
        factor[block_position, block_position] = jnp.sqrt(running)
        for i in range(block_position + 1, size):
            running = gram[i, block_position]
            for k in range(block_position):
                running = running - factor[i, k] * factor[block_position, k]
            factor[i, block_position] = running / factor[block_position, block_position]
    forward = []
    for i in range(size):
        running = target[i]
        for k in range(i):
            running = running - factor[i, k] * forward[k]
        forward.append(running / factor[i, i])
    analysis_output = [None] * size
    for i in reversed(range(size)):
        running = forward[i]
        for k in range(i + 1, size):
            running = running - factor[k, i] * analysis_output[k]
        analysis_output[i] = running / factor[i, i]
    return jnp.stack(analysis_output)


def previous_blocks(entry_values, reach_devices):
    pieces = [
        from_behind(entry_values, ("region", "blk"), shift_by)
        for shift_by in range(reach_devices, 0, -1)
    ]
    return jnp.concatenate(pieces, axis=0)


def on_device(ensemble, observed, obs_var, ridge, pred_back, bounds):
    highest = lax.Precision.HIGHEST
    local_blocks, rows, members = ensemble.shape
    slots = pred_back.shape[1]
    reach_devices = -(-REACH // local_blocks)
    before = reach_devices * local_blocks
    anomaly = (ensemble - jnp.mean(ensemble, axis=2, keepdims=True)) / jnp.sqrt(
        jnp.float32(members - 1)
    )
    positions = before + jnp.arange(local_blocks, dtype=jnp.int32)[:, None] - pred_back
    positions = jnp.where(pred_back > 0, positions, before + local_blocks)
    empty_zero_matrix = jnp.zeros((1, rows, members), jnp.float32)

    def extend(entry_values):
        return jnp.concatenate(
            [previous_blocks(entry_values, reach_devices), entry_values, empty_zero_matrix], axis=0
        )

    preds = extend(anomaly)[positions]
    identity = jnp.eye(slots, dtype=jnp.float32)
    gram = jnp.einsum("bjrm,bkrm->jkbr", preds, preds, precision=highest)
    gram = gram + ridge[None, None, :, None] * identity[:, :, None, None]
    target = jnp.einsum("bjrm,brm->jbr", preds, anomaly, precision=highest)
    regression_coefficients = small_solve(gram, target)
    resid = anomaly - jnp.einsum("jbr,bjrm->brm", regression_coefficients, preds, precision=highest)
    inverse_var = 1.0 / (jnp.sum(resid * resid, axis=2) + 1e-05)
    inverse_obs = 1.0 / obs_var
    beta_blocks = jnp.transpose(regression_coefficients, (1, 0, 2))
    lower_bound = bounds[0]
    upper_bound = bounds[1]
    theta = (upper_bound + lower_bound) / 2
    delta = (upper_bound - lower_bound) / 2
    sigma = theta / delta
    rho_now = 1.0 / sigma
    residue = inverse_obs[:, :, None] * (observed - ensemble)
    increment = jnp.zeros_like(ensemble)
    direction = residue / theta
    for step in range(ITERS):
        increment = increment + direction
        extended = extend(direction)
        lower_analysis_output = direction
        for lower_slot in range(slots):
            lower_analysis_output = (
                lower_analysis_output
                - beta_blocks[:, lower_slot, :, None] * extended[positions[:, lower_slot]]
            )
        upper_entry_values = lower_analysis_output * inverse_var[:, :, None]
        window = jnp.zeros((before + local_blocks + 1, rows, members), jnp.float32)
        for slot in range(slots):
            window = window.at[positions[:, slot]].add(
                beta_blocks[:, slot, :, None] * upper_entry_values
            )
        analysis_output = upper_entry_values - window[before : before + local_blocks]
        for shift_by in range(1, reach_devices + 1):
            start = (reach_devices - shift_by) * local_blocks
            analysis_output = analysis_output - from_behind(
                window[start : start + local_blocks], ("region", "blk"), -shift_by
            )
        residue = residue - (analysis_output + inverse_obs[:, :, None] * direction)
        rho_next = 1.0 / (2 * sigma - rho_now)
        direction = rho_next * rho_now * direction + 2 * rho_next / delta * residue
        rho_now = rho_next
    increment = increment + direction
    return ensemble + increment


SUB = 8
LANES = 128
MESH_ID = pl.DeviceIdType.MESH


def place():
    per = lax.axis_size("blk")
    me = lax.axis_index("region") * per + lax.axis_index("blk")
    return per, me


def greet(n, per, me):
    barrier = pltpu.get_barrier_semaphore()

    def signal(i, carry):
        k = lax.rem(me + i, n)
        pl.semaphore_signal(
            barrier, inc=1, device_id=(k // per, lax.rem(k, per)), device_id_type=MESH_ID
        )
        return carry

    lax.fori_loop(1, n, signal, 0)
    pl.semaphore_wait(barrier, n - 1)


def copy_to(src, dst, send_sem, recv_sem, k, per):
    return pltpu.make_async_remote_copy(
        src_ref=src,
        dst_ref=dst,
        send_sem=send_sem,
        recv_sem=recv_sem,
        device_id=(k // per, lax.rem(k, per)),
        device_id_type=MESH_ID,
    )


def to_rows_kernel(n, ens, obs, pack, ens_r, obs_r, pack_r, send_sem, recv_sem):
    per, me = place()
    local = ens.shape[0]
    greet(n, per, me)
    mine = pl.ds(me * local, local)

    def send_ens(i, carry):
        k = lax.rem(me + i, n)
        rows = pl.ds(pl.multiple_of(k * SUB, SUB), SUB)
        copy_to(ens.at[:, rows, :], ens_r.at[mine], send_sem.at[0], recv_sem.at[0], k, per).start()
        return carry

    def send_rest(i, carry):
        k = lax.rem(me + i, n)
        rows = pl.ds(pl.multiple_of(k * SUB, SUB), SUB)
        copy_to(pack.at[k], pack_r.at[mine], send_sem.at[1], recv_sem.at[1], k, per).start()
        copy_to(obs.at[:, rows, :], obs_r.at[mine], send_sem.at[2], recv_sem.at[2], k, per).start()
        return carry

    lax.fori_loop(1, n, send_ens, 0)
    lax.fori_loop(1, n, send_rest, 0)
    own = pl.ds(pl.multiple_of(me * SUB, SUB), SUB)
    ens_r[mine] = ens[:, own, :]
    obs_r[mine] = obs[:, own, :]
    pack_r[mine] = pack[me]
    other = lax.rem(me + 1, n)
    sent = pl.ds(0, (n - 1) * SUB)
    got = pl.ds(0, (n - 1) * local)
    for which, (a, b) in enumerate(
        (
            (ens.at[:, sent, :], ens_r.at[got]),
            (pack.at[pl.ds(0, n - 1)], pack_r.at[got]),
            (obs.at[:, sent, :], obs_r.at[got]),
        )
    ):
        copy_to(b, b, send_sem.at[which], recv_sem.at[which], other, per).wait_recv()
        copy_to(a, a, send_sem.at[which], recv_sem.at[which], other, per).wait_send()


def to_blocks_kernel(n, z_r, z, send_sem, recv_sem):
    per, me = place()
    local = z.shape[0]
    greet(n, per, me)
    own = pl.ds(pl.multiple_of(me * SUB, SUB), SUB)

    def send(i, carry):
        k = lax.rem(me + i, n)
        copy_to(
            z_r.at[pl.ds(k * local, local)], z.at[:, own, :], send_sem, recv_sem, k, per
        ).start()
        return carry

    lax.fori_loop(1, n, send, 0)
    z[:, own, :] = z_r[pl.ds(me * local, local)]
    other = lax.rem(me + 1, n)
    a = z_r.at[pl.ds(0, (n - 1) * local)]
    b = z.at[:, pl.ds(0, (n - 1) * SUB), :]
    copy_to(b, b, send_sem, recv_sem, other, per).wait_recv()
    copy_to(a, a, send_sem, recv_sem, other, per).wait_send()


def rows_kernel(nb, bounds, ens, obs, pack, z, apad, dpad, upad, res, ivar, iobs, corr, wide):
    members = ens.shape[2]
    tile = (SUB, LANES)
    zero = jnp.zeros(tile, jnp.float32)
    for i in range(REACH):
        apad[i] = zero
        dpad[i] = zero
        upad[nb + i] = zero
    x = ens[...]
    mean = jnp.sum(x, axis=2, keepdims=True) * (1.0 / members)
    apad[pl.ds(REACH, nb)] = (x - mean) * (1.0 / math.sqrt(members - 1))

    lane = lax.broadcasted_iota(jnp.int32, (nb, LANES), 1)
    back = lane - lax.broadcasted_iota(jnp.int32, (nb, LANES), 0)
    for r in range(SUB):
        lhs = apad[pl.ds(REACH, nb), r, :]
        rhs = jnp.concatenate([lhs, jnp.zeros((LANES - nb, members), jnp.float32)], axis=0)
        full = lax.dot_general(
            lhs,
            rhs,
            (((1,), (1,)), ((), ())),
            precision=lax.Precision.HIGHEST,
            preferred_element_type=jnp.float32,
        )
        for delta in range(REACH + 1):
            corr[delta, r : r + 1, :] = jnp.sum(
                jnp.where(back == delta, full, 0.0), axis=0, keepdims=True
            )

    flat = pack[...].reshape(nb, LANES)
    turned = jnp.concatenate([flat, jnp.zeros((LANES - nb, LANES), jnp.float32)], axis=0).T
    obs_rows = turned[0:SUB]
    on_lane = lax.broadcasted_iota(jnp.int32, tile, 1)
    chosen = [
        jnp.broadcast_to(turned[SUB + d : SUB + d + 1], tile) > 0.5 for d in range(REACH)
    ]
    at = SUB + REACH
    ridge = jnp.where(on_lane < nb, jnp.broadcast_to(turned[at : at + 1], tile), 1.0)

    factor = {}
    inverse = []
    for j in range(REACH):
        for i in range(j, REACH):
            value = pltpu.roll(corr[i - j], j + 1, 1)
            running = jnp.where(chosen[j], jnp.where(chosen[i], value, 0.0), 0.0)
            if i == j:
                running = running + ridge
            for k in range(j):
                running = running - factor[i, k] * factor[j, k]
            if i == j:
                inverse.append(1.0 / jnp.sqrt(running))
            else:
                factor[i, j] = running * inverse[j]
    forward = []
    for i in range(REACH):
        running = jnp.where(chosen[i], corr[i + 1], 0.0)
        for k in range(i):
            running = running - factor[i, k] * forward[k]
        forward.append(running * inverse[i])
    beta = [None] * REACH
    for i in reversed(range(REACH)):
        running = forward[i]
        for k in range(i + 1, REACH):
            running = running - factor[k, i] * beta[k]
        beta[i] = running * inverse[i]
    for d in range(REACH):
        for g in range(nb + REACH):
            wide[g, d] = jnp.broadcast_to(beta[d][:, g : g + 1], tile) if g < nb else zero
    inverse_obs = 1.0 / jnp.where(on_lane < nb, obs_rows, 1.0)
    for g in range(nb):
        iobs[g] = jnp.broadcast_to(inverse_obs[:, g : g + 1], tile)

    def lower(ref, g0):
        values = [ref[g0 + i] for i in range(REACH + SUB)]
        outs = []
        for g in range(SUB):
            total = values[REACH + g]
            for d in range(REACH):
                total = total - wide[g0 + g, d] * values[REACH + g - d - 1]
            outs.append(total)
        return outs

    def upper(ref, g0):
        values = [ref[g0 + i] for i in range(REACH + SUB)]
        outs = []
        for g in range(SUB):
            total = values[g]
            for d in range(REACH):
                total = total - wide[g0 + g + d + 1, d] * values[g + d + 1]
            outs.append(total)
        return outs

    lo = jnp.full(tile, bounds[0], jnp.float32)
    hi = jnp.full(tile, bounds[1], jnp.float32)
    theta = (hi + lo) / 2
    delta = (hi - lo) / 2
    sigma = theta / delta
    rho = 1.0 / sigma

    def start(t, carry):
        g0 = t * SUB
        for g, resid in enumerate(lower(apad, g0)):
            total = jnp.sum(resid * resid, axis=1, keepdims=True) + 1e-05
            ivar[g0 + g] = jnp.broadcast_to(1.0 / total, tile)
            rhs = iobs[g0 + g] * (obs[g0 + g] - ens[g0 + g])
            res[g0 + g] = rhs
            first = rhs / theta
            dpad[REACH + g0 + g] = first
            z[g0 + g] = first
        return carry

    lax.fori_loop(0, nb // SUB, start, 0)
    for step in range(ITERS):
        rho_next = 1.0 / (2 * sigma - rho)
        keep = rho_next * rho
        move = 2 * rho_next / delta
        rho = rho_next

        def down(t, carry):
            g0 = t * SUB
            for g, value in enumerate(lower(dpad, g0)):
                upad[g0 + g] = value * ivar[g0 + g]
            return carry

        def up(t, carry):
            g0 = t * SUB
            for g, value in enumerate(upper(upad, g0)):
                old = dpad[REACH + g0 + g]
                left = res[g0 + g] - (value + iobs[g0 + g] * old)
                fresh = keep * old + move * left
                res[g0 + g] = left
                dpad[REACH + g0 + g] = fresh
                z[g0 + g] = z[g0 + g] + fresh
            return carry

        lax.fori_loop(0, nb // SUB, down, 0)
        lax.fori_loop(0, nb // SUB, up, 0)


def by_rows(n, ensemble, observed, obs_var, ridge, pred_back, bounds):
    local, rows, members = ensemble.shape
    nb = n * local
    f32 = jnp.float32
    distance = jnp.arange(1, REACH + 1, dtype=jnp.int32)
    chosen = jnp.any(pred_back[:, None, :] == distance[None, :, None], axis=2).astype(f32)
    pack = jnp.concatenate(
        [
            jnp.transpose(obs_var.reshape(local, n, SUB), (1, 0, 2)),
            jnp.broadcast_to(chosen[None], (n, local, REACH)),
            jnp.broadcast_to(ridge[None, :, None], (n, local, 1)),
            jnp.zeros((n, local, LANES - SUB - REACH - 1), f32),
        ],
        axis=2,
    ).reshape(n, local, 1, LANES)
    vmem = pl.BlockSpec(memory_space=pltpu.VMEM)
    row_shape = jax.ShapeDtypeStruct((nb, SUB, members), f32)
    ens_r, obs_r, pack_r = pl.pallas_call(
        functools.partial(to_rows_kernel, n),
        out_shape=(row_shape, row_shape, jax.ShapeDtypeStruct((nb, 1, LANES), f32)),
        in_specs=[vmem] * 3,
        out_specs=(vmem,) * 3,
        scratch_shapes=[pltpu.SemaphoreType.DMA((3,)), pltpu.SemaphoreType.DMA((3,))],
        compiler_params=pltpu.CompilerParams(collective_id=0, has_side_effects=True),
        name="to_rows",
    )(ensemble, observed, pack)
    blocks = lambda count: pltpu.VMEM((count, SUB, members), f32)
    z_r = pl.pallas_call(
        functools.partial(rows_kernel, nb),
        out_shape=row_shape,
        in_specs=[pl.BlockSpec(memory_space=pltpu.SMEM)] + [vmem] * 3,
        out_specs=vmem,
        scratch_shapes=[
            blocks(nb + REACH),
            blocks(nb + REACH),
            blocks(nb + REACH),
            blocks(nb),
            blocks(nb),
            blocks(nb),
            pltpu.VMEM((REACH + 1, SUB, LANES), f32),
            pltpu.VMEM((nb + REACH, REACH, SUB, LANES), f32),
        ],
        compiler_params=pltpu.CompilerParams(vmem_limit_bytes=48 << 20),
        name="rows",
    )(bounds, ens_r, obs_r, pack_r)
    z = pl.pallas_call(
        functools.partial(to_blocks_kernel, n),
        out_shape=jax.ShapeDtypeStruct(ensemble.shape, f32),
        in_specs=[vmem],
        out_specs=vmem,
        scratch_shapes=[pltpu.SemaphoreType.DMA, pltpu.SemaphoreType.DMA],
        compiler_params=pltpu.CompilerParams(collective_id=1, has_side_effects=True),
        name="to_blocks",
    )(z_r)
    return ensemble + z


def choose(n, ensemble, *rest):
    local, rows, members = ensemble.shape
    fits = rows == n * SUB and members == LANES and n * local + REACH <= LANES
    if fits and (n * local) % SUB == 0:
        return by_rows(n, ensemble, *rest)
    return on_device(ensemble, *rest)


def solution(mesh):
    return jax.shard_map(
        functools.partial(choose, mesh.size),
        mesh=mesh,
        in_specs=(
            P(("region", "blk"), None, None),
            P(("region", "blk"), None, None),
            P(("region", "blk"), None),
            P(("region", "blk")),
            P(("region", "blk"), None),
            P(),
        ),
        out_specs=P(("region", "blk"), None, None),
        check_vma=False,
    )
```

```python
import functools
import math

import jax
import jax.numpy as jnp
from jax import lax
from jax.experimental import pallas as pl
from jax.experimental.pallas import tpu as pltpu
from jax.sharding import PartitionSpec as P

REACH = 16
ITERS = 3


def from_behind(value, axis, steps):
    count = lax.axis_size(axis)
    first, last = (max(0, -steps), min(count, count - steps))
    return lax.ppermute(value, axis, [(source, source + steps) for source in range(first, last)])


def small_solve(gram, target):
    size = gram.shape[0]
    factor = {}
    for block_position in range(size):
        running = gram[block_position, block_position]
        for k in range(block_position):
            running = running - factor[block_position, k] * factor[block_position, k]
        factor[block_position, block_position] = jnp.sqrt(running)
        for i in range(block_position + 1, size):
            running = gram[i, block_position]
            for k in range(block_position):
                running = running - factor[i, k] * factor[block_position, k]
            factor[i, block_position] = running / factor[block_position, block_position]
    forward = []
    for i in range(size):
        running = target[i]
        for k in range(i):
            running = running - factor[i, k] * forward[k]
        forward.append(running / factor[i, i])
    analysis_output = [None] * size
    for i in reversed(range(size)):
        running = forward[i]
        for k in range(i + 1, size):
            running = running - factor[k, i] * analysis_output[k]
        analysis_output[i] = running / factor[i, i]
    return jnp.stack(analysis_output)


def previous_blocks(entry_values, reach_devices):
    pieces = [
        from_behind(entry_values, ("region", "blk"), shift_by)
        for shift_by in range(reach_devices, 0, -1)
    ]
    return jnp.concatenate(pieces, axis=0)


def on_device(ensemble, observed, obs_var, ridge, pred_back, bounds):
    highest = lax.Precision.HIGHEST
    local_blocks, rows, members = ensemble.shape
    slots = pred_back.shape[1]
    reach_devices = -(-REACH // local_blocks)
    before = reach_devices * local_blocks
    anomaly = (ensemble - jnp.mean(ensemble, axis=2, keepdims=True)) / jnp.sqrt(
        jnp.float32(members - 1)
    )
    positions = before + jnp.arange(local_blocks, dtype=jnp.int32)[:, None] - pred_back
    positions = jnp.where(pred_back > 0, positions, before + local_blocks)
    empty_zero_matrix = jnp.zeros((1, rows, members), jnp.float32)

    def extend(entry_values):
        return jnp.concatenate(
            [previous_blocks(entry_values, reach_devices), entry_values, empty_zero_matrix], axis=0
        )

    preds = extend(anomaly)[positions]
    identity = jnp.eye(slots, dtype=jnp.float32)
    gram = jnp.einsum("bjrm,bkrm->jkbr", preds, preds, precision=highest)
    gram = gram + ridge[None, None, :, None] * identity[:, :, None, None]
    target = jnp.einsum("bjrm,brm->jbr", preds, anomaly, precision=highest)
    regression_coefficients = small_solve(gram, target)
    resid = anomaly - jnp.einsum("jbr,bjrm->brm", regression_coefficients, preds, precision=highest)
    inverse_var = 1.0 / (jnp.sum(resid * resid, axis=2) + 1e-05)
    inverse_obs = 1.0 / obs_var
    beta_blocks = jnp.transpose(regression_coefficients, (1, 0, 2))
    lower_bound = bounds[0]
    upper_bound = bounds[1]
    theta = (upper_bound + lower_bound) / 2
    delta = (upper_bound - lower_bound) / 2
    sigma = theta / delta
    rho_now = 1.0 / sigma
    residue = inverse_obs[:, :, None] * (observed - ensemble)
    increment = jnp.zeros_like(ensemble)
    direction = residue / theta
    for step in range(ITERS):
        increment = increment + direction
        extended = extend(direction)
        lower_analysis_output = direction
        for lower_slot in range(slots):
            lower_analysis_output = (
                lower_analysis_output
                - beta_blocks[:, lower_slot, :, None] * extended[positions[:, lower_slot]]
            )
        upper_entry_values = lower_analysis_output * inverse_var[:, :, None]
        window = jnp.zeros((before + local_blocks + 1, rows, members), jnp.float32)
        for slot in range(slots):
            window = window.at[positions[:, slot]].add(
                beta_blocks[:, slot, :, None] * upper_entry_values
            )
        analysis_output = upper_entry_values - window[before : before + local_blocks]
        for shift_by in range(1, reach_devices + 1):
            start = (reach_devices - shift_by) * local_blocks
            analysis_output = analysis_output - from_behind(
                window[start : start + local_blocks], ("region", "blk"), -shift_by
            )
        residue = residue - (analysis_output + inverse_obs[:, :, None] * direction)
        rho_next = 1.0 / (2 * sigma - rho_now)
        direction = rho_next * rho_now * direction + 2 * rho_next / delta * residue
        rho_now = rho_next
    increment = increment + direction
    return ensemble + increment


SUB = 8
LANES = 128
MESH_ID = pl.DeviceIdType.MESH


def place():
    per = lax.axis_size("blk")
    me = lax.axis_index("region") * per + lax.axis_index("blk")
    return per, me


def greet(n, per, me):
    barrier = pltpu.get_barrier_semaphore()

    def signal(i, carry):
        k = lax.rem(me + i, n)
        pl.semaphore_signal(
            barrier, inc=1, device_id=(k // per, lax.rem(k, per)), device_id_type=MESH_ID
        )
        return carry

    lax.fori_loop(1, n, signal, 0)
    pl.semaphore_wait(barrier, n - 1)


def copy_to(src, dst, send_sem, recv_sem, k, per):
    return pltpu.make_async_remote_copy(
        src_ref=src,
        dst_ref=dst,
        send_sem=send_sem,
        recv_sem=recv_sem,
        device_id=(k // per, lax.rem(k, per)),
        device_id_type=MESH_ID,
    )


def gather_rows(n, per, me, ens, obs, obs_var, ridge, pred_back, pack, ens_r, obs_r, pack_r, sems):
    send_sem, recv_sem = sems
    local, rows, members = ens.shape
    mine = pl.ds(me * local, local)

    def send_ens(i, carry):
        k = lax.rem(me + i, n)
        part = pl.ds(pl.multiple_of(k * SUB, SUB), SUB)
        copy_to(ens.at[:, part, :], ens_r.at[mine], send_sem.at[0], recv_sem.at[0], k, per).start()
        return carry

    lax.fori_loop(1, n, send_ens, 0)

    lane = lax.broadcasted_iota(jnp.int32, (1, LANES), 1)
    groups = LANES // SUB
    for block in range(local):
        meta = jnp.where(lane == SUB + REACH, ridge[block], 0.0)
        for slot in range(pred_back.shape[1]):
            back = pred_back[block, slot]
            meta = jnp.where((lane == back + (SUB - 1)) & (lane >= SUB), 1.0, meta)
        for half in range(rows // LANES):
            row = obs_var[block : block + 1, half * LANES : (half + 1) * LANES]
            for k in range(groups):
                turned = row if k == 0 else pltpu.roll(row, LANES - SUB * k, 1)
                pack[half * groups + k, block] = jnp.where(lane < SUB, turned, meta)

    def send_pack(i, carry):
        k = lax.rem(me + i, n)
        copy_to(pack.at[k], pack_r.at[mine], send_sem.at[1], recv_sem.at[1], k, per).start()
        return carry

    lax.fori_loop(1, n, send_pack, 0)

    def send_obs(i, carry):
        k = lax.rem(me + i, n)
        part = pl.ds(pl.multiple_of(k * SUB, SUB), SUB)
        copy_to(obs.at[:, part, :], obs_r.at[mine], send_sem.at[2], recv_sem.at[2], k, per).start()
        return carry

    lax.fori_loop(1, n, send_obs, 0)
    own = pl.ds(pl.multiple_of(me * SUB, SUB), SUB)
    ens_r[mine] = ens[:, own, :]
    obs_r[mine] = obs[:, own, :]
    pack_r[mine] = pack[me]


def whole_kernel(
    n, bounds, ens, obs, obs_var, ridge, pred_back, z,
    pack, ens_r, obs_r, pack_r, z_r, send_sem, recv_sem,
    apad, dpad, upad, res, ivar, iobs, corr, wide,
):
    per, me = place()
    local = ens.shape[0]
    greet(n, per, me)
    gather_rows(
        n, per, me, ens, obs, obs_var, ridge, pred_back, pack, ens_r, obs_r, pack_r,
        (send_sem, recv_sem),
    )
    other = lax.rem(me + 1, n)
    sent = pl.ds(0, (n - 1) * SUB)
    got = pl.ds(0, (n - 1) * local)
    whole = (
        (ens.at[:, sent, :], ens_r.at[got]),
        (pack.at[pl.ds(0, n - 1)], pack_r.at[got]),
        (obs.at[:, sent, :], obs_r.at[got]),
        (z_r.at[got], z.at[:, sent, :]),
    )

    def arrived(which):
        ref = whole[which][1]
        copy_to(ref, ref, send_sem.at[which], recv_sem.at[which], other, per).wait_recv()

    rows_part(
        n * local, arrived, bounds, ens_r, obs_r, pack_r, z_r,
        apad, dpad, upad, res, ivar, iobs, corr, wide,
    )
    own = pl.ds(pl.multiple_of(me * SUB, SUB), SUB)

    def send(i, carry):
        k = lax.rem(me + i, n)
        copy_to(
            z_r.at[pl.ds(k * local, local)], z.at[:, own, :], send_sem.at[3], recv_sem.at[3], k, per
        ).start()
        return carry

    lax.fori_loop(1, n, send, 0)
    z[:, own, :] = z_r[pl.ds(me * local, local)]
    arrived(3)
    for which, (ref, unused) in enumerate(whole):
        copy_to(ref, ref, send_sem.at[which], recv_sem.at[which], other, per).wait_send()


def rows_part(nb, arrived, bounds, ens, obs, pack, z, apad, dpad, upad, res, ivar, iobs, corr, wide):
    members = ens.shape[2]
    tile = (SUB, LANES)
    zero = jnp.zeros(tile, jnp.float32)
    for i in range(REACH):
        apad[i] = zero
        dpad[i] = zero
        upad[nb + i] = zero
    arrived(0)
    x = ens[...]
    mean = jnp.sum(x, axis=2, keepdims=True) * (1.0 / members)
    apad[pl.ds(REACH, nb)] = (x - mean) * (1.0 / math.sqrt(members - 1))

    lane = lax.broadcasted_iota(jnp.int32, (nb, LANES), 1)
    back = lane - lax.broadcasted_iota(jnp.int32, (nb, LANES), 0)
    for r in range(SUB):
        lhs = apad[pl.ds(REACH, nb), r, :]
        rhs = jnp.concatenate([lhs, jnp.zeros((LANES - nb, members), jnp.float32)], axis=0)
        full = lax.dot_general(
            lhs,
            rhs,
            (((1,), (1,)), ((), ())),
            precision=lax.Precision.HIGHEST,
            preferred_element_type=jnp.float32,
        )
        for delta in range(REACH + 1):
            corr[delta, r : r + 1, :] = jnp.sum(
                jnp.where(back == delta, full, 0.0), axis=0, keepdims=True
            )

    arrived(1)
    flat = pack[...].reshape(nb, LANES)
    turned = jnp.concatenate([flat, jnp.zeros((LANES - nb, LANES), jnp.float32)], axis=0).T
    obs_rows = turned[0:SUB]
    on_lane = lax.broadcasted_iota(jnp.int32, tile, 1)
    chosen = [
        jnp.broadcast_to(turned[SUB + d : SUB + d + 1], tile) > 0.5 for d in range(REACH)
    ]
    at = SUB + REACH
    ridge = jnp.where(on_lane < nb, jnp.broadcast_to(turned[at : at + 1], tile), 1.0)

    factor = {}
    inverse = []
    for j in range(REACH):
        for i in range(j, REACH):
            value = pltpu.roll(corr[i - j], j + 1, 1)
            running = jnp.where(chosen[j], jnp.where(chosen[i], value, 0.0), 0.0)
            if i == j:
                running = running + ridge
            for k in range(j):
                running = running - factor[i, k] * factor[j, k]
            if i == j:
                inverse.append(1.0 / jnp.sqrt(running))
            else:
                factor[i, j] = running * inverse[j]
    forward = []
    for i in range(REACH):
        running = jnp.where(chosen[i], corr[i + 1], 0.0)
        for k in range(i):
            running = running - factor[i, k] * forward[k]
        forward.append(running * inverse[i])
    beta = [None] * REACH
    for i in reversed(range(REACH)):
        running = forward[i]
        for k in range(i + 1, REACH):
            running = running - factor[k, i] * beta[k]
        beta[i] = running * inverse[i]
    for d in range(REACH):
        for g in range(nb + REACH):
            wide[g, d] = jnp.broadcast_to(beta[d][:, g : g + 1], tile) if g < nb else zero
    inverse_obs = 1.0 / jnp.where(on_lane < nb, obs_rows, 1.0)
    for g in range(nb):
        iobs[g] = jnp.broadcast_to(inverse_obs[:, g : g + 1], tile)

    def lower(ref, g0):
        values = [ref[g0 + i] for i in range(REACH + SUB)]
        outs = []
        for g in range(SUB):
            total = values[REACH + g]
            for d in range(REACH):
                total = total - wide[g0 + g, d] * values[REACH + g - d - 1]
            outs.append(total)
        return outs

    def upper(ref, g0):
        values = [ref[g0 + i] for i in range(REACH + SUB)]
        outs = []
        for g in range(SUB):
            total = values[g]
            for d in range(REACH):
                total = total - wide[g0 + g + d + 1, d] * values[g + d + 1]
            outs.append(total)
        return outs

    arrived(2)
    lo = jnp.full(tile, bounds[0], jnp.float32)
    hi = jnp.full(tile, bounds[1], jnp.float32)
    theta = (hi + lo) / 2
    delta = (hi - lo) / 2
    sigma = theta / delta
    rho = 1.0 / sigma

    def start(t, carry):
        g0 = t * SUB
        for g, resid in enumerate(lower(apad, g0)):
            total = jnp.sum(resid * resid, axis=1, keepdims=True) + 1e-05
            ivar[g0 + g] = jnp.broadcast_to(1.0 / total, tile)
            rhs = iobs[g0 + g] * (obs[g0 + g] - ens[g0 + g])
            res[g0 + g] = rhs
            first = rhs / theta
            dpad[REACH + g0 + g] = first
            z[g0 + g] = first
        return carry

    lax.fori_loop(0, nb // SUB, start, 0)
    for step in range(ITERS):
        rho_next = 1.0 / (2 * sigma - rho)
        keep = rho_next * rho
        move = 2 * rho_next / delta
        rho = rho_next

        def down(t, carry):
            g0 = t * SUB
            for g, value in enumerate(lower(dpad, g0)):
                upad[g0 + g] = value * ivar[g0 + g]
            return carry

        def up(t, carry):
            g0 = t * SUB
            for g, value in enumerate(upper(upad, g0)):
                old = dpad[REACH + g0 + g]
                left = res[g0 + g] - (value + iobs[g0 + g] * old)
                fresh = keep * old + move * left
                res[g0 + g] = left
                dpad[REACH + g0 + g] = fresh
                z[g0 + g] = z[g0 + g] + fresh
            return carry

        lax.fori_loop(0, nb // SUB, down, 0)
        lax.fori_loop(0, nb // SUB, up, 0)


def by_rows(n, ensemble, observed, obs_var, ridge, pred_back, bounds):
    local, rows, members = ensemble.shape
    nb = n * local
    f32 = jnp.float32
    vmem = pl.BlockSpec(memory_space=pltpu.VMEM)
    smem = pl.BlockSpec(memory_space=pltpu.SMEM)
    blocks = lambda count: pltpu.VMEM((count, SUB, members), f32)
    z = pl.pallas_call(
        functools.partial(whole_kernel, n),
        out_shape=jax.ShapeDtypeStruct(ensemble.shape, f32),
        in_specs=[smem, vmem, vmem, vmem, smem, smem],
        out_specs=vmem,
        scratch_shapes=[
            pltpu.VMEM((n, local, 1, LANES), f32),
            blocks(nb),
            blocks(nb),
            pltpu.VMEM((nb, 1, LANES), f32),
            blocks(nb),
            pltpu.SemaphoreType.DMA((4,)),
            pltpu.SemaphoreType.DMA((4,)),
            blocks(nb + REACH),
            blocks(nb + REACH),
            blocks(nb + REACH),
            blocks(nb),
            blocks(nb),
            blocks(nb),
            pltpu.VMEM((REACH + 1, SUB, LANES), f32),
            pltpu.VMEM((nb + REACH, REACH, SUB, LANES), f32),
        ],
        compiler_params=pltpu.CompilerParams(
            collective_id=0, has_side_effects=True, vmem_limit_bytes=48 << 20
        ),
        name="whole",
    )(bounds, ensemble, observed, obs_var, ridge, pred_back)
    return ensemble + z


def choose(n, ensemble, *rest):
    local, rows, members = ensemble.shape
    fits = rows == n * SUB and members == LANES and n * local + REACH <= LANES
    if fits and (n * local) % SUB == 0:
        return by_rows(n, ensemble, *rest)
    return on_device(ensemble, *rest)


def solution(mesh):
    return jax.shard_map(
        functools.partial(choose, mesh.size),
        mesh=mesh,
        in_specs=(
            P(("region", "blk"), None, None),
            P(("region", "blk"), None, None),
            P(("region", "blk"), None),
            P(("region", "blk")),
            P(("region", "blk"), None),
            P(),
        ),
        out_specs=P(("region", "blk"), None, None),
        check_vma=False,
    )
```

```python
import functools
import math

import jax
import jax.numpy as jnp
from jax import lax
from jax.experimental import pallas as pl
from jax.experimental.pallas import tpu as pltpu
from jax.sharding import PartitionSpec as P

REACH = 16
ITERS = 3


def from_behind(value, axis, steps):
    count = lax.axis_size(axis)
    first, last = (max(0, -steps), min(count, count - steps))
    return lax.ppermute(value, axis, [(source, source + steps) for source in range(first, last)])


def small_solve(gram, target):
    size = gram.shape[0]
    factor = {}
    for block_position in range(size):
        running = gram[block_position, block_position]
        for k in range(block_position):
            running = running - factor[block_position, k] * factor[block_position, k]
        factor[block_position, block_position] = jnp.sqrt(running)
        for i in range(block_position + 1, size):
            running = gram[i, block_position]
            for k in range(block_position):
                running = running - factor[i, k] * factor[block_position, k]
            factor[i, block_position] = running / factor[block_position, block_position]
    forward = []
    for i in range(size):
        running = target[i]
        for k in range(i):
            running = running - factor[i, k] * forward[k]
        forward.append(running / factor[i, i])
    analysis_output = [None] * size
    for i in reversed(range(size)):
        running = forward[i]
        for k in range(i + 1, size):
            running = running - factor[k, i] * analysis_output[k]
        analysis_output[i] = running / factor[i, i]
    return jnp.stack(analysis_output)


def previous_blocks(entry_values, reach_devices):
    pieces = [
        from_behind(entry_values, ("region", "blk"), shift_by)
        for shift_by in range(reach_devices, 0, -1)
    ]
    return jnp.concatenate(pieces, axis=0)


def on_device(ensemble, observed, obs_var, ridge, pred_back, bounds):
    highest = lax.Precision.HIGHEST
    local_blocks, rows, members = ensemble.shape
    slots = pred_back.shape[1]
    reach_devices = -(-REACH // local_blocks)
    before = reach_devices * local_blocks
    anomaly = (ensemble - jnp.mean(ensemble, axis=2, keepdims=True)) / jnp.sqrt(
        jnp.float32(members - 1)
    )
    positions = before + jnp.arange(local_blocks, dtype=jnp.int32)[:, None] - pred_back
    positions = jnp.where(pred_back > 0, positions, before + local_blocks)
    empty_zero_matrix = jnp.zeros((1, rows, members), jnp.float32)

    def extend(entry_values):
        return jnp.concatenate(
            [previous_blocks(entry_values, reach_devices), entry_values, empty_zero_matrix], axis=0
        )

    preds = extend(anomaly)[positions]
    identity = jnp.eye(slots, dtype=jnp.float32)
    gram = jnp.einsum("bjrm,bkrm->jkbr", preds, preds, precision=highest)
    gram = gram + ridge[None, None, :, None] * identity[:, :, None, None]
    target = jnp.einsum("bjrm,brm->jbr", preds, anomaly, precision=highest)
    regression_coefficients = small_solve(gram, target)
    resid = anomaly - jnp.einsum("jbr,bjrm->brm", regression_coefficients, preds, precision=highest)
    inverse_var = 1.0 / (jnp.sum(resid * resid, axis=2) + 1e-05)
    inverse_obs = 1.0 / obs_var
    beta_blocks = jnp.transpose(regression_coefficients, (1, 0, 2))
    lower_bound = bounds[0]
    upper_bound = bounds[1]
    theta = (upper_bound + lower_bound) / 2
    delta = (upper_bound - lower_bound) / 2
    sigma = theta / delta
    rho_now = 1.0 / sigma
    residue = inverse_obs[:, :, None] * (observed - ensemble)
    increment = jnp.zeros_like(ensemble)
    direction = residue / theta
    for step in range(ITERS):
        increment = increment + direction
        extended = extend(direction)
        lower_analysis_output = direction
        for lower_slot in range(slots):
            lower_analysis_output = (
                lower_analysis_output
                - beta_blocks[:, lower_slot, :, None] * extended[positions[:, lower_slot]]
            )
        upper_entry_values = lower_analysis_output * inverse_var[:, :, None]
        window = jnp.zeros((before + local_blocks + 1, rows, members), jnp.float32)
        for slot in range(slots):
            window = window.at[positions[:, slot]].add(
                beta_blocks[:, slot, :, None] * upper_entry_values
            )
        analysis_output = upper_entry_values - window[before : before + local_blocks]
        for shift_by in range(1, reach_devices + 1):
            start = (reach_devices - shift_by) * local_blocks
            analysis_output = analysis_output - from_behind(
                window[start : start + local_blocks], ("region", "blk"), -shift_by
            )
        residue = residue - (analysis_output + inverse_obs[:, :, None] * direction)
        rho_next = 1.0 / (2 * sigma - rho_now)
        direction = rho_next * rho_now * direction + 2 * rho_next / delta * residue
        rho_now = rho_next
    increment = increment + direction
    return ensemble + increment


VMEM_GRANT = 66_700_000
SUB = 8
LANES = 128
MESH_ID = pl.DeviceIdType.MESH


def place():
    per = lax.axis_size("blk")
    me = lax.axis_index("region") * per + lax.axis_index("blk")
    return per, me


def greet(n, per, me):
    barrier = pltpu.get_barrier_semaphore()

    def signal(i, carry):
        k = lax.rem(me + i, n)
        pl.semaphore_signal(
            barrier, inc=1, device_id=(k // per, lax.rem(k, per)), device_id_type=MESH_ID
        )
        return carry

    lax.fori_loop(1, n, signal, 0)
    pl.semaphore_wait(barrier, n - 1)


def copy_to(src, dst, send_sem, recv_sem, k, per):
    return pltpu.make_async_remote_copy(
        src_ref=src,
        dst_ref=dst,
        send_sem=send_sem,
        recv_sem=recv_sem,
        device_id=(k // per, lax.rem(k, per)),
        device_id_type=MESH_ID,
    )


def gather_rows(n, per, me, loads, ens, obs, obs_var, ridge, pred_back, pack, ens_r, obs_r, pack_r, sems):
    send_sem, recv_sem = sems
    local, rows, members = ens.shape
    mine = pl.ds(me * local, local)

    def send_ens(i, carry):
        k = lax.rem(me + i, n)
        part = pl.ds(pl.multiple_of(k * SUB, SUB), SUB)
        copy_to(ens.at[:, part, :], ens_r.at[mine], send_sem.at[0], recv_sem.at[0], k, per).start()
        return carry

    loads[0].wait()
    lax.fori_loop(1, n, send_ens, 0)
    for load in loads[1:]:
        load.wait()

    lane = lax.broadcasted_iota(jnp.int32, (1, LANES), 1)
    groups = LANES // SUB
    for block in range(local):
        meta = jnp.where(lane == SUB + REACH, ridge[block], 0.0)
        for slot in range(pred_back.shape[1]):
            back = pred_back[block, slot]
            meta = jnp.where((lane == back + (SUB - 1)) & (lane >= SUB), 1.0, meta)
        for half in range(rows // LANES):
            row = obs_var[block : block + 1, half * LANES : (half + 1) * LANES]
            for k in range(groups):
                turned = row if k == 0 else pltpu.roll(row, LANES - SUB * k, 1)
                pack[half * groups + k, block] = jnp.where(lane < SUB, turned, meta)

    def send_pack(i, carry):
        k = lax.rem(me + i, n)
        copy_to(pack.at[k], pack_r.at[mine], send_sem.at[1], recv_sem.at[1], k, per).start()
        return carry

    lax.fori_loop(1, n, send_pack, 0)

    def send_obs(i, carry):
        k = lax.rem(me + i, n)
        part = pl.ds(pl.multiple_of(k * SUB, SUB), SUB)
        copy_to(obs.at[:, part, :], obs_r.at[mine], send_sem.at[2], recv_sem.at[2], k, per).start()
        return carry

    lax.fori_loop(1, n, send_obs, 0)
    own = pl.ds(pl.multiple_of(me * SUB, SUB), SUB)
    ens_r[mine] = ens[:, own, :]
    obs_r[mine] = obs[:, own, :]
    pack_r[mine] = pack[me]


def whole_kernel(
    n, bounds_in, ens_in, obs_in, obs_var_in, ridge_in, pred_back_in, z,
    bounds, ens, obs, obs_var, ridge, pred_back, load_sem, pack, ens_r, obs_r, pack_r, z_r, send_sem, recv_sem,
    apad, dpad, upad, res, ivar, iobs, corr, wide,
):
    per, me = place()
    local = ens.shape[0]
    loads = [
        pltpu.make_async_copy(src, dst, load_sem.at[i])
        for i, (src, dst) in enumerate(
            (
                (ens_in, ens),
                (obs_in, obs),
                (obs_var_in, obs_var),
                (ridge_in, ridge),
                (pred_back_in, pred_back),
                (bounds_in, bounds),
            )
        )
    ]
    for load in loads:
        load.start()
    greet(n, per, me)
    gather_rows(
        n, per, me, loads, ens, obs, obs_var, ridge, pred_back, pack, ens_r, obs_r, pack_r,
        (send_sem, recv_sem),
    )
    other = lax.rem(me + 1, n)
    sent = pl.ds(0, (n - 1) * SUB)
    got = pl.ds(0, (n - 1) * local)
    whole = (
        (ens.at[:, sent, :], ens_r.at[got]),
        (pack.at[pl.ds(0, n - 1)], pack_r.at[got]),
        (obs.at[:, sent, :], obs_r.at[got]),
        (z_r.at[got], z.at[:, sent, :]),
    )

    def arrived(which):
        ref = whole[which][1]
        copy_to(ref, ref, send_sem.at[which], recv_sem.at[which], other, per).wait_recv()

    rows_part(
        n * local, arrived, bounds, ens_r, obs_r, pack_r, z_r,
        apad, dpad, upad, res, ivar, iobs, corr, wide,
    )
    own = pl.ds(pl.multiple_of(me * SUB, SUB), SUB)

    def send(i, carry):
        k = lax.rem(me + i, n)
        copy_to(
            z_r.at[pl.ds(k * local, local)], z.at[:, own, :], send_sem.at[3], recv_sem.at[3], k, per
        ).start()
        return carry

    lax.fori_loop(1, n, send, 0)
    z[:, own, :] = z_r[pl.ds(me * local, local)]
    arrived(3)
    for which, (ref, unused) in enumerate(whole):
        copy_to(ref, ref, send_sem.at[which], recv_sem.at[which], other, per).wait_send()


def rows_part(nb, arrived, bounds, ens, obs, pack, z, apad, dpad, upad, res, ivar, iobs, corr, wide):
    members = ens.shape[2]
    tile = (SUB, LANES)
    zero = jnp.zeros(tile, jnp.float32)
    for i in range(REACH):
        apad[i] = zero
        dpad[i] = zero
        upad[nb + i] = zero
    arrived(0)
    x = ens[...]
    mean = jnp.sum(x, axis=2, keepdims=True) * (1.0 / members)
    apad[pl.ds(REACH, nb)] = (x - mean) * (1.0 / math.sqrt(members - 1))

    lane = lax.broadcasted_iota(jnp.int32, (nb, LANES), 1)
    back = lane - lax.broadcasted_iota(jnp.int32, (nb, LANES), 0)
    for r in range(SUB):
        lhs = apad[pl.ds(REACH, nb), r, :]
        rhs = jnp.concatenate([lhs, jnp.zeros((LANES - nb, members), jnp.float32)], axis=0)
        full = lax.dot_general(
            lhs,
            rhs,
            (((1,), (1,)), ((), ())),
            precision=lax.Precision.HIGHEST,
            preferred_element_type=jnp.float32,
        )
        for delta in range(REACH + 1):
            corr[delta, r : r + 1, :] = jnp.sum(
                jnp.where(back == delta, full, 0.0), axis=0, keepdims=True
            )

    arrived(1)
    flat = pack[...].reshape(nb, LANES)
    turned = jnp.concatenate([flat, jnp.zeros((LANES - nb, LANES), jnp.float32)], axis=0).T
    obs_rows = turned[0:SUB]
    on_lane = lax.broadcasted_iota(jnp.int32, tile, 1)
    chosen = [
        jnp.broadcast_to(turned[SUB + d : SUB + d + 1], tile) > 0.5 for d in range(REACH)
    ]
    at = SUB + REACH
    ridge = jnp.where(on_lane < nb, jnp.broadcast_to(turned[at : at + 1], tile), 1.0)

    factor = {}
    inverse = []
    for j in range(REACH):
        for i in range(j, REACH):
            value = pltpu.roll(corr[i - j], j + 1, 1)
            running = jnp.where(chosen[j], jnp.where(chosen[i], value, 0.0), 0.0)
            if i == j:
                running = running + ridge
            for k in range(j):
                running = running - factor[i, k] * factor[j, k]
            if i == j:
                inverse.append(1.0 / jnp.sqrt(running))
            else:
                factor[i, j] = running * inverse[j]
    forward = []
    for i in range(REACH):
        running = jnp.where(chosen[i], corr[i + 1], 0.0)
        for k in range(i):
            running = running - factor[i, k] * forward[k]
        forward.append(running * inverse[i])
    beta = [None] * REACH
    for i in reversed(range(REACH)):
        running = forward[i]
        for k in range(i + 1, REACH):
            running = running - factor[k, i] * beta[k]
        beta[i] = running * inverse[i]
    for d in range(REACH):
        for g in range(nb + REACH):
            wide[g, d] = jnp.broadcast_to(beta[d][:, g : g + 1], tile) if g < nb else zero
    inverse_obs = 1.0 / jnp.where(on_lane < nb, obs_rows, 1.0)
    for g in range(nb):
        iobs[g] = jnp.broadcast_to(inverse_obs[:, g : g + 1], tile)

    def lower(ref, g0):
        values = [ref[g0 + i] for i in range(REACH + SUB)]
        outs = []
        for g in range(SUB):
            total = values[REACH + g]
            for d in range(REACH):
                total = total - wide[g0 + g, d] * values[REACH + g - d - 1]
            outs.append(total)
        return outs

    def upper(ref, g0):
        values = [ref[g0 + i] for i in range(REACH + SUB)]
        outs = []
        for g in range(SUB):
            total = values[g]
            for d in range(REACH):
                total = total - wide[g0 + g + d + 1, d] * values[g + d + 1]
            outs.append(total)
        return outs

    arrived(2)
    lo = jnp.full(tile, bounds[0], jnp.float32)
    hi = jnp.full(tile, bounds[1], jnp.float32)
    theta = (hi + lo) / 2
    delta = (hi - lo) / 2
    sigma = theta / delta
    rho = 1.0 / sigma

    def start(t, carry):
        g0 = t * SUB
        for g, resid in enumerate(lower(apad, g0)):
            total = jnp.sum(resid * resid, axis=1, keepdims=True) + 1e-05
            ivar[g0 + g] = jnp.broadcast_to(1.0 / total, tile)
            rhs = iobs[g0 + g] * (obs[g0 + g] - ens[g0 + g])
            res[g0 + g] = rhs
            first = rhs / theta
            dpad[REACH + g0 + g] = first
            z[g0 + g] = first
        return carry

    lax.fori_loop(0, nb // SUB, start, 0)
    for step in range(ITERS):
        rho_next = 1.0 / (2 * sigma - rho)
        keep = rho_next * rho
        move = 2 * rho_next / delta
        rho = rho_next

        def down(t, carry):
            g0 = t * SUB
            for g, value in enumerate(lower(dpad, g0)):
                upad[g0 + g] = value * ivar[g0 + g]
            return carry

        def up(t, carry):
            g0 = t * SUB
            for g, value in enumerate(upper(upad, g0)):
                old = dpad[REACH + g0 + g]
                left = res[g0 + g] - (value + iobs[g0 + g] * old)
                fresh = keep * old + move * left
                res[g0 + g] = left
                dpad[REACH + g0 + g] = fresh
                z[g0 + g] = z[g0 + g] + fresh
            return carry

        lax.fori_loop(0, nb // SUB, down, 0)
        lax.fori_loop(0, nb // SUB, up, 0)


def by_rows(n, ensemble, observed, obs_var, ridge, pred_back, bounds):
    local, rows, members = ensemble.shape
    nb = n * local
    f32 = jnp.float32
    vmem = pl.BlockSpec(memory_space=pltpu.VMEM)
    hbm = pl.BlockSpec(memory_space=pltpu.HBM)
    blocks = lambda count: pltpu.VMEM((count, SUB, members), f32)
    z = pl.pallas_call(
        functools.partial(whole_kernel, n),
        out_shape=jax.ShapeDtypeStruct(ensemble.shape, f32),
        in_specs=[hbm] * 6,
        out_specs=vmem,
        scratch_shapes=[
            pltpu.SMEM(bounds.shape, f32),
            pltpu.VMEM(ensemble.shape, f32),
            pltpu.VMEM(observed.shape, f32),
            pltpu.VMEM(obs_var.shape, f32),
            pltpu.SMEM(ridge.shape, f32),
            pltpu.SMEM(pred_back.shape, jnp.int32),
            pltpu.SemaphoreType.DMA((6,)),
            pltpu.VMEM((n, local, 1, LANES), f32),
            blocks(nb),
            blocks(nb),
            pltpu.VMEM((nb, 1, LANES), f32),
            blocks(nb),
            pltpu.SemaphoreType.DMA((4,)),
            pltpu.SemaphoreType.DMA((4,)),
            blocks(nb + REACH),
            blocks(nb + REACH),
            blocks(nb + REACH),
            blocks(nb),
            blocks(nb),
            blocks(nb),
            pltpu.VMEM((REACH + 1, SUB, LANES), f32),
            pltpu.VMEM((nb + REACH, REACH, SUB, LANES), f32),
        ],
        compiler_params=pltpu.CompilerParams(
            collective_id=0, has_side_effects=True, vmem_limit_bytes=VMEM_GRANT
        ),
        name="whole",
    )(bounds, ensemble, observed, obs_var, ridge, pred_back)
    return ensemble + z


def choose(n, ensemble, *rest):
    local, rows, members = ensemble.shape
    fits = rows == n * SUB and members == LANES and n * local + REACH <= LANES
    if fits and (n * local) % SUB == 0:
        return by_rows(n, ensemble, *rest)
    return on_device(ensemble, *rest)


def solution(mesh):
    return jax.shard_map(
        functools.partial(choose, mesh.size),
        mesh=mesh,
        in_specs=(
            P(("region", "blk"), None, None),
            P(("region", "blk"), None, None),
            P(("region", "blk"), None),
            P(("region", "blk")),
            P(("region", "blk"), None),
            P(),
        ),
        out_specs=P(("region", "blk"), None, None),
        check_vma=False,
    )
```

```python
import functools
import math

import jax
import jax.numpy as jnp
from jax import lax
from jax.experimental import pallas as pl
from jax.experimental.pallas import tpu as pltpu
from jax.sharding import PartitionSpec as P

REACH = 16
ITERS = 3


def from_behind(value, axis, steps):
    count = lax.axis_size(axis)
    first, last = (max(0, -steps), min(count, count - steps))
    return lax.ppermute(value, axis, [(source, source + steps) for source in range(first, last)])


def small_solve(gram, target):
    size = gram.shape[0]
    factor = {}
    for block_position in range(size):
        running = gram[block_position, block_position]
        for k in range(block_position):
            running = running - factor[block_position, k] * factor[block_position, k]
        factor[block_position, block_position] = jnp.sqrt(running)
        for i in range(block_position + 1, size):
            running = gram[i, block_position]
            for k in range(block_position):
                running = running - factor[i, k] * factor[block_position, k]
            factor[i, block_position] = running / factor[block_position, block_position]
    forward = []
    for i in range(size):
        running = target[i]
        for k in range(i):
            running = running - factor[i, k] * forward[k]
        forward.append(running / factor[i, i])
    analysis_output = [None] * size
    for i in reversed(range(size)):
        running = forward[i]
        for k in range(i + 1, size):
            running = running - factor[k, i] * analysis_output[k]
        analysis_output[i] = running / factor[i, i]
    return jnp.stack(analysis_output)


def previous_blocks(entry_values, reach_devices):
    pieces = [
        from_behind(entry_values, ("region", "blk"), shift_by)
        for shift_by in range(reach_devices, 0, -1)
    ]
    return jnp.concatenate(pieces, axis=0)


def on_device(ensemble, observed, obs_var, ridge, pred_back, bounds):
    highest = lax.Precision.HIGHEST
    local_blocks, rows, members = ensemble.shape
    slots = pred_back.shape[1]
    reach_devices = -(-REACH // local_blocks)
    before = reach_devices * local_blocks
    anomaly = (ensemble - jnp.mean(ensemble, axis=2, keepdims=True)) / jnp.sqrt(
        jnp.float32(members - 1)
    )
    positions = before + jnp.arange(local_blocks, dtype=jnp.int32)[:, None] - pred_back
    positions = jnp.where(pred_back > 0, positions, before + local_blocks)
    empty_zero_matrix = jnp.zeros((1, rows, members), jnp.float32)

    def extend(entry_values):
        return jnp.concatenate(
            [previous_blocks(entry_values, reach_devices), entry_values, empty_zero_matrix], axis=0
        )

    preds = extend(anomaly)[positions]
    identity = jnp.eye(slots, dtype=jnp.float32)
    gram = jnp.einsum("bjrm,bkrm->jkbr", preds, preds, precision=highest)
    gram = gram + ridge[None, None, :, None] * identity[:, :, None, None]
    target = jnp.einsum("bjrm,brm->jbr", preds, anomaly, precision=highest)
    regression_coefficients = small_solve(gram, target)
    resid = anomaly - jnp.einsum("jbr,bjrm->brm", regression_coefficients, preds, precision=highest)
    inverse_var = 1.0 / (jnp.sum(resid * resid, axis=2) + 1e-05)
    inverse_obs = 1.0 / obs_var
    beta_blocks = jnp.transpose(regression_coefficients, (1, 0, 2))
    lower_bound = bounds[0]
    upper_bound = bounds[1]
    theta = (upper_bound + lower_bound) / 2
    delta = (upper_bound - lower_bound) / 2
    sigma = theta / delta
    rho_now = 1.0 / sigma
    residue = inverse_obs[:, :, None] * (observed - ensemble)
    increment = jnp.zeros_like(ensemble)
    direction = residue / theta
    for step in range(ITERS):
        increment = increment + direction
        extended = extend(direction)
        lower_analysis_output = direction
        for lower_slot in range(slots):
            lower_analysis_output = (
                lower_analysis_output
                - beta_blocks[:, lower_slot, :, None] * extended[positions[:, lower_slot]]
            )
        upper_entry_values = lower_analysis_output * inverse_var[:, :, None]
        window = jnp.zeros((before + local_blocks + 1, rows, members), jnp.float32)
        for slot in range(slots):
            window = window.at[positions[:, slot]].add(
                beta_blocks[:, slot, :, None] * upper_entry_values
            )
        analysis_output = upper_entry_values - window[before : before + local_blocks]
        for shift_by in range(1, reach_devices + 1):
            start = (reach_devices - shift_by) * local_blocks
            analysis_output = analysis_output - from_behind(
                window[start : start + local_blocks], ("region", "blk"), -shift_by
            )
        residue = residue - (analysis_output + inverse_obs[:, :, None] * direction)
        rho_next = 1.0 / (2 * sigma - rho_now)
        direction = rho_next * rho_now * direction + 2 * rho_next / delta * residue
        rho_now = rho_next
    increment = increment + direction
    return ensemble + increment


VMEM_GRANT = 66_700_000
SUB = 8
LANES = 128
MESH_ID = pl.DeviceIdType.MESH


def place():
    per = lax.axis_size("blk")
    me = lax.axis_index("region") * per + lax.axis_index("blk")
    return per, me


def greet(n, per, me):
    barrier = pltpu.get_barrier_semaphore()

    def signal(i, carry):
        k = lax.rem(me + i, n)
        pl.semaphore_signal(
            barrier, inc=1, device_id=(k // per, lax.rem(k, per)), device_id_type=MESH_ID
        )
        return carry

    lax.fori_loop(1, n, signal, 0)
    pl.semaphore_wait(barrier, n - 1)


def copy_to(src, dst, send_sem, recv_sem, k, per):
    return pltpu.make_async_remote_copy(
        src_ref=src,
        dst_ref=dst,
        send_sem=send_sem,
        recv_sem=recv_sem,
        device_id=(k // per, lax.rem(k, per)),
        device_id_type=MESH_ID,
    )


def partners(n, per, me):
    bits = [(1 << b, lax.rem(me // (1 << b), 2)) for b in range(n.bit_length() - 1)]
    keep = [weight * bit for weight, bit in bits]
    flip = [weight * (1 - bit) for weight, bit in bits]
    for i in sorted(range(1, n), key=lambda i: (-(i % per), -i)):
        yield sum(flip[b] if (i >> b) & 1 else keep[b] for b in range(len(bits)))


def gather_rows(n, per, me, loads, ens, obs, obs_var, ridge, pred_back, pack, ens_r, obs_r, pack_r, sems):
    send_sem, recv_sem = sems
    local, rows, members = ens.shape
    mine = pl.ds(me * local, local)

    loads[0].wait()
    for k in partners(n, per, me):
        part = pl.ds(pl.multiple_of(k * SUB, SUB), SUB)
        copy_to(ens.at[:, part, :], ens_r.at[mine], send_sem.at[0], recv_sem.at[0], k, per).start()
    for load in loads[1:]:
        load.wait()

    lane = lax.broadcasted_iota(jnp.int32, (1, LANES), 1)
    groups = LANES // SUB
    for block in range(local):
        meta = jnp.where(lane == SUB + REACH, ridge[block], 0.0)
        for slot in range(pred_back.shape[1]):
            back = pred_back[block, slot]
            meta = jnp.where((lane == back + (SUB - 1)) & (lane >= SUB), 1.0, meta)
        for half in range(rows // LANES):
            row = obs_var[block : block + 1, half * LANES : (half + 1) * LANES]
            for k in range(groups):
                turned = row if k == 0 else pltpu.roll(row, LANES - SUB * k, 1)
                pack[half * groups + k, block] = jnp.where(lane < SUB, turned, meta)

    for k in partners(n, per, me):
        copy_to(pack.at[k], pack_r.at[mine], send_sem.at[1], recv_sem.at[1], k, per).start()

    for k in partners(n, per, me):
        part = pl.ds(pl.multiple_of(k * SUB, SUB), SUB)
        copy_to(obs.at[:, part, :], obs_r.at[mine], send_sem.at[2], recv_sem.at[2], k, per).start()
    own = pl.ds(pl.multiple_of(me * SUB, SUB), SUB)
    ens_r[mine] = ens[:, own, :]
    obs_r[mine] = obs[:, own, :]
    pack_r[mine] = pack[me]


def whole_kernel(
    n, bounds_in, ens_in, obs_in, obs_var_in, ridge_in, pred_back_in, z,
    bounds, ens, obs, obs_var, ridge, pred_back, load_sem, pack, ens_r, obs_r, pack_r, z_r, send_sem, recv_sem,
    apad, dpad, upad, res, ivar, iobs, corr, wide,
):
    per, me = place()
    local = ens.shape[0]
    loads = [
        pltpu.make_async_copy(src, dst, load_sem.at[i])
        for i, (src, dst) in enumerate(
            (
                (ens_in, ens),
                (obs_in, obs),
                (obs_var_in, obs_var),
                (ridge_in, ridge),
                (pred_back_in, pred_back),
                (bounds_in, bounds),
            )
        )
    ]
    for load in loads:
        load.start()
    greet(n, per, me)
    gather_rows(
        n, per, me, loads, ens, obs, obs_var, ridge, pred_back, pack, ens_r, obs_r, pack_r,
        (send_sem, recv_sem),
    )
    other = lax.rem(me + 1, n)
    sent = pl.ds(0, (n - 1) * SUB)
    got = pl.ds(0, (n - 1) * local)
    whole = (
        (ens.at[:, sent, :], ens_r.at[got]),
        (pack.at[pl.ds(0, n - 1)], pack_r.at[got]),
        (obs.at[:, sent, :], obs_r.at[got]),
        (z_r.at[got], z.at[:, sent, :]),
    )

    def arrived(which):
        ref = whole[which][1]
        copy_to(ref, ref, send_sem.at[which], recv_sem.at[which], other, per).wait_recv()

    rows_part(
        n * local, arrived, bounds, ens_r, obs_r, pack_r, z_r,
        apad, dpad, upad, res, ivar, iobs, corr, wide,
    )
    own = pl.ds(pl.multiple_of(me * SUB, SUB), SUB)

    for k in partners(n, per, me):
        copy_to(
            z_r.at[pl.ds(k * local, local)], z.at[:, own, :], send_sem.at[3], recv_sem.at[3], k, per
        ).start()
    z[:, own, :] = z_r[pl.ds(me * local, local)]
    arrived(3)
    for which, (ref, unused) in enumerate(whole):
        copy_to(ref, ref, send_sem.at[which], recv_sem.at[which], other, per).wait_send()


def rows_part(nb, arrived, bounds, ens, obs, pack, z, apad, dpad, upad, res, ivar, iobs, corr, wide):
    members = ens.shape[2]
    tile = (SUB, LANES)
    zero = jnp.zeros(tile, jnp.float32)
    for i in range(REACH):
        apad[i] = zero
        dpad[i] = zero
        upad[nb + i] = zero
    arrived(0)
    x = ens[...]
    mean = jnp.sum(x, axis=2, keepdims=True) * (1.0 / members)
    apad[pl.ds(REACH, nb)] = (x - mean) * (1.0 / math.sqrt(members - 1))

    lane = lax.broadcasted_iota(jnp.int32, (nb, LANES), 1)
    back = lane - lax.broadcasted_iota(jnp.int32, (nb, LANES), 0)
    for r in range(SUB):
        lhs = apad[pl.ds(REACH, nb), r, :]
        rhs = jnp.concatenate([lhs, jnp.zeros((LANES - nb, members), jnp.float32)], axis=0)
        full = lax.dot_general(
            lhs,
            rhs,
            (((1,), (1,)), ((), ())),
            precision=lax.Precision.HIGHEST,
            preferred_element_type=jnp.float32,
        )
        for delta in range(REACH + 1):
            corr[delta, r : r + 1, :] = jnp.sum(
                jnp.where(back == delta, full, 0.0), axis=0, keepdims=True
            )

    arrived(1)
    flat = pack[...].reshape(nb, LANES)
    turned = jnp.concatenate([flat, jnp.zeros((LANES - nb, LANES), jnp.float32)], axis=0).T
    obs_rows = turned[0:SUB]
    on_lane = lax.broadcasted_iota(jnp.int32, tile, 1)
    chosen = [
        jnp.broadcast_to(turned[SUB + d : SUB + d + 1], tile) > 0.5 for d in range(REACH)
    ]
    at = SUB + REACH
    ridge = jnp.where(on_lane < nb, jnp.broadcast_to(turned[at : at + 1], tile), 1.0)

    factor = {}
    inverse = []
    for j in range(REACH):
        for i in range(j, REACH):
            value = pltpu.roll(corr[i - j], j + 1, 1)
            running = jnp.where(chosen[j], jnp.where(chosen[i], value, 0.0), 0.0)
            if i == j:
                running = running + ridge
            for k in range(j):
                running = running - factor[i, k] * factor[j, k]
            if i == j:
                inverse.append(1.0 / jnp.sqrt(running))
            else:
                factor[i, j] = running * inverse[j]
    forward = []
    for i in range(REACH):
        running = jnp.where(chosen[i], corr[i + 1], 0.0)
        for k in range(i):
            running = running - factor[i, k] * forward[k]
        forward.append(running * inverse[i])
    beta = [None] * REACH
    for i in reversed(range(REACH)):
        running = forward[i]
        for k in range(i + 1, REACH):
            running = running - factor[k, i] * beta[k]
        beta[i] = running * inverse[i]
    for d in range(REACH):
        for g in range(nb + REACH):
            wide[g, d] = jnp.broadcast_to(beta[d][:, g : g + 1], tile) if g < nb else zero
    inverse_obs = 1.0 / jnp.where(on_lane < nb, obs_rows, 1.0)
    for g in range(nb):
        iobs[g] = jnp.broadcast_to(inverse_obs[:, g : g + 1], tile)

    def lower(ref, g0):
        values = [ref[g0 + i] for i in range(REACH + SUB)]
        outs = []
        for g in range(SUB):
            total = values[REACH + g]
            for d in range(REACH):
                total = total - wide[g0 + g, d] * values[REACH + g - d - 1]
            outs.append(total)
        return outs

    def upper(ref, g0):
        values = [ref[g0 + i] for i in range(REACH + SUB)]
        outs = []
        for g in range(SUB):
            total = values[g]
            for d in range(REACH):
                total = total - wide[g0 + g + d + 1, d] * values[g + d + 1]
            outs.append(total)
        return outs

    arrived(2)
    lo = jnp.full(tile, bounds[0], jnp.float32)
    hi = jnp.full(tile, bounds[1], jnp.float32)
    theta = (hi + lo) / 2
    delta = (hi - lo) / 2
    sigma = theta / delta
    rho = 1.0 / sigma

    def start(t, carry):
        g0 = t * SUB
        for g, resid in enumerate(lower(apad, g0)):
            total = jnp.sum(resid * resid, axis=1, keepdims=True) + 1e-05
            ivar[g0 + g] = jnp.broadcast_to(1.0 / total, tile)
            rhs = iobs[g0 + g] * (obs[g0 + g] - ens[g0 + g])
            res[g0 + g] = rhs
            first = rhs / theta
            dpad[REACH + g0 + g] = first
            z[g0 + g] = first
        return carry

    lax.fori_loop(0, nb // SUB, start, 0)
    for step in range(ITERS):
        rho_next = 1.0 / (2 * sigma - rho)
        keep = rho_next * rho
        move = 2 * rho_next / delta
        rho = rho_next

        def down(t, carry):
            g0 = t * SUB
            for g, value in enumerate(lower(dpad, g0)):
                upad[g0 + g] = value * ivar[g0 + g]
            return carry

        def up(t, carry):
            g0 = t * SUB
            for g, value in enumerate(upper(upad, g0)):
                old = dpad[REACH + g0 + g]
                left = res[g0 + g] - (value + iobs[g0 + g] * old)
                fresh = keep * old + move * left
                res[g0 + g] = left
                dpad[REACH + g0 + g] = fresh
                z[g0 + g] = z[g0 + g] + fresh
            return carry

        lax.fori_loop(0, nb // SUB, down, 0)
        lax.fori_loop(0, nb // SUB, up, 0)


def by_rows(n, ensemble, observed, obs_var, ridge, pred_back, bounds):
    local, rows, members = ensemble.shape
    nb = n * local
    f32 = jnp.float32
    vmem = pl.BlockSpec(memory_space=pltpu.VMEM)
    hbm = pl.BlockSpec(memory_space=pltpu.HBM)
    blocks = lambda count: pltpu.VMEM((count, SUB, members), f32)
    z = pl.pallas_call(
        functools.partial(whole_kernel, n),
        out_shape=jax.ShapeDtypeStruct(ensemble.shape, f32),
        in_specs=[hbm] * 6,
        out_specs=vmem,
        scratch_shapes=[
            pltpu.SMEM(bounds.shape, f32),
            pltpu.VMEM(ensemble.shape, f32),
            pltpu.VMEM(observed.shape, f32),
            pltpu.VMEM(obs_var.shape, f32),
            pltpu.SMEM(ridge.shape, f32),
            pltpu.SMEM(pred_back.shape, jnp.int32),
            pltpu.SemaphoreType.DMA((6,)),
            pltpu.VMEM((n, local, 1, LANES), f32),
            blocks(nb),
            blocks(nb),
            pltpu.VMEM((nb, 1, LANES), f32),
            blocks(nb),
            pltpu.SemaphoreType.DMA((4,)),
            pltpu.SemaphoreType.DMA((4,)),
            blocks(nb + REACH),
            blocks(nb + REACH),
            blocks(nb + REACH),
            blocks(nb),
            blocks(nb),
            blocks(nb),
            pltpu.VMEM((REACH + 1, SUB, LANES), f32),
            pltpu.VMEM((nb + REACH, REACH, SUB, LANES), f32),
        ],
        compiler_params=pltpu.CompilerParams(
            collective_id=0, has_side_effects=True, vmem_limit_bytes=VMEM_GRANT
        ),
        name="whole",
    )(bounds, ensemble, observed, obs_var, ridge, pred_back)
    return ensemble + z


def choose(n, ensemble, *rest):
    local, rows, members = ensemble.shape
    fits = rows == n * SUB and members == LANES and n * local + REACH <= LANES
    if fits and (n * local) % SUB == 0 and n & (n - 1) == 0:
        return by_rows(n, ensemble, *rest)
    return on_device(ensemble, *rest)


def solution(mesh):
    return jax.shard_map(
        functools.partial(choose, mesh.size),
        mesh=mesh,
        in_specs=(
            P(("region", "blk"), None, None),
            P(("region", "blk"), None, None),
            P(("region", "blk"), None),
            P(("region", "blk")),
            P(("region", "blk"), None),
            P(),
        ),
        out_specs=P(("region", "blk"), None, None),
        check_vma=False,
    )
```
